32 devices in a mesh: dp: 4 (over x, y), tp: 8 (over z, core).
Axes of the slice: x: 2, y: 2, z: 4, core: 2. Of those that a mesh axis runs over, the one named last changes fastest.
Arguments:
- hidden: bfloat16 [4, 128, 5120], P('dp', 'tp'), parts along dimension 0
- norm_attn: float32 [2, 5120], replicated
- w_q: bfloat16 [2, 5120, 40, 128], P(None, None, 'tp')
- w_kv: bfloat16 [2, 5120, 2, 8, 128], replicated
- w_o: bfloat16 [2, 40, 128, 5120], P(None, 'tp')
- norm_mlp: float32 [2, 5120], replicated
- w_gate: bfloat16 [2, 5120, 13824], P(None, None, 'tp')
- w_up: bfloat16 [2, 5120, 13824], P(None, None, 'tp')
- w_down: bfloat16 [2, 13824, 5120], P(None, 'tp')
Outputs:
- output: bfloat16 [4, 128, 5120], P('dp', 'tp'), parts along dimension 0
There are 4 independent parts. The reference program is written for one: setup_inputs(seed, part) draws one part's arguments, and reference() takes and returns one part's arrays. A program takes and returns all parts, laid end to end along the dimension named above; an argument that names none is the same for every part.
All inputs are finite; a program needn't handle non-finite values.
Results may differ from the reference program's by a relative error of at most 0.0109612.
Values are sent between devices in bfloat16 or wider.
A program may use at most 1 GiB of HBM per device.

```python
import math
import jax
import jax.numpy as jnp
from jax import lax

D = 5120
HEADS = 40
KV_HEADS = 8
HEAD = 128
FF = 13824
BATCH = 1
SEQ = 128
LAYERS = 2

EPS = 1e-5
ROPE_BASE = 10000.0
GROUP = HEADS // KV_HEADS


def setup_inputs(seed: int = 0, part: int = 0) -> dict:
    root = jax.random.key(seed)
    keys = jax.random.split(root, 9)
    tok_key, scale_key = jax.random.split(jax.random.fold_in(keys[8], part))
    tokens = jax.random.normal(tok_key, (BATCH, SEQ, D), jnp.float32)
    tok_scale = jax.random.uniform(scale_key, (BATCH, SEQ, 1), jnp.float32, 0.5, 2.0)
    hidden = (tokens * tok_scale).astype(jnp.bfloat16)
    qk_gain = math.sqrt(math.sqrt(math.log(max(SEQ / 8.0, 4.0))))
    in_scale = 1.0 / math.sqrt(D)
    out_scale = 1.0 / math.sqrt(HEADS * HEAD)
    ff_scale = 1.0 / math.sqrt(FF)
    norm_attn = 1.0 + 0.3 * jax.random.uniform(keys[0], (LAYERS, D), jnp.float32, -1.0, 1.0)
    w_q = (jax.random.normal(keys[1], (LAYERS, D, HEADS, HEAD), jnp.float32) * (in_scale * qk_gain)).astype(jnp.bfloat16)
    kv_gain = jnp.array([qk_gain, 1.0], jnp.float32).reshape(1, 1, 2, 1, 1)
    w_kv = (jax.random.normal(keys[2], (LAYERS, D, 2, KV_HEADS, HEAD), jnp.float32) * in_scale * kv_gain).astype(jnp.bfloat16)
    w_o = (jax.random.normal(keys[3], (LAYERS, HEADS, HEAD, D), jnp.float32) * out_scale).astype(jnp.bfloat16)
    norm_mlp = 1.0 + 0.3 * jax.random.uniform(keys[4], (LAYERS, D), jnp.float32, -1.0, 1.0)
    w_gate = (jax.random.normal(keys[5], (LAYERS, D, FF), jnp.float32) * in_scale).astype(jnp.bfloat16)
    w_up = (jax.random.normal(keys[6], (LAYERS, D, FF), jnp.float32) * in_scale).astype(jnp.bfloat16)
    w_down = (jax.random.normal(keys[7], (LAYERS, FF, D), jnp.float32) * ff_scale).astype(jnp.bfloat16)
    return {'hidden': hidden, 'norm_attn': norm_attn, 'w_q': w_q, 'w_kv': w_kv, 'w_o': w_o, 'norm_mlp': norm_mlp, 'w_gate': w_gate, 'w_up': w_up, 'w_down': w_down}


def rms_norm(resid, gain):
    mean_sq = jnp.mean(resid * resid, axis=-1, keepdims=True)
    return (resid * lax.rsqrt(mean_sq + EPS) * gain).astype(jnp.bfloat16)


def rope_tables(positions, head_dim):
    half_dim = head_dim // 2
    inv_freq = jnp.power(ROPE_BASE, -2.0 * jnp.arange(half_dim, dtype=jnp.float32) / head_dim)
    angles = positions.astype(jnp.float32)[:, None] * inv_freq[None, :]
    return jnp.cos(angles), jnp.sin(angles)


def apply_rope(proj, cos_t, sin_t):
    half_dim = proj.shape[-1] // 2
    first_half = proj[..., :half_dim]
    second_half = proj[..., half_dim:]
    cos_b = cos_t[:, None, :]
    sin_b = sin_t[:, None, :]
    return jnp.concatenate([first_half * cos_b - second_half * sin_b, second_half * cos_b + first_half * sin_b], axis=-1)


def decoder_layer(resid, layer_w, cos_t, sin_t, causal_mask):
    attn_gain, q_weight, kv_weight, o_weight, mlp_gain, gate_weight, up_weight, down_weight = layer_w
    normed = rms_norm(resid, attn_gain)
    q_proj = jnp.dot(normed, q_weight.reshape(D, HEADS * HEAD), preferred_element_type=jnp.float32).reshape(SEQ, HEADS, HEAD)
    kv_proj = jnp.dot(normed, kv_weight.reshape(D, 2 * KV_HEADS * HEAD), preferred_element_type=jnp.float32).reshape(SEQ, 2, KV_HEADS, HEAD)
    queries = apply_rope(q_proj, cos_t, sin_t).astype(jnp.bfloat16)
    keys = apply_rope(kv_proj[:, 0], cos_t, sin_t).astype(jnp.bfloat16)
    values = kv_proj[:, 1].astype(jnp.bfloat16)
    q_heads = jnp.transpose(queries, (1, 0, 2))
    k_heads = jnp.repeat(jnp.transpose(keys, (1, 0, 2)), GROUP, axis=0)
    v_heads = jnp.repeat(jnp.transpose(values, (1, 0, 2)), GROUP, axis=0)
    inv_sqrt = 1.0 / math.sqrt(HEAD)

    def attend(head_args):
        q_one, k_one, v_one = head_args
        scores = jnp.dot(q_one, k_one.T, preferred_element_type=jnp.float32) * inv_sqrt
        scores = jnp.where(causal_mask, scores, -jnp.inf)
        attn_probs = jax.nn.softmax(scores, axis=-1).astype(jnp.bfloat16)
        return jnp.dot(attn_probs, v_one, preferred_element_type=jnp.float32).astype(jnp.bfloat16)

    context = lax.map(attend, (q_heads, k_heads, v_heads))
    context = jnp.transpose(context, (1, 0, 2)).reshape(SEQ, HEADS * HEAD)
    resid = resid + jnp.dot(context, o_weight.reshape(HEADS * HEAD, D), preferred_element_type=jnp.float32)
    normed = rms_norm(resid, mlp_gain)
    gate_proj = jnp.dot(normed, gate_weight, preferred_element_type=jnp.float32)
    up_proj = jnp.dot(normed, up_weight, preferred_element_type=jnp.float32)
    activated = (jax.nn.silu(gate_proj) * up_proj).astype(jnp.bfloat16)
    return resid + jnp.dot(activated, down_weight, preferred_element_type=jnp.float32)


def reference(hidden, norm_attn, w_q, w_kv, w_o, norm_mlp, w_gate, w_up, w_down):
    positions = jnp.arange(SEQ)
    cos_t, sin_t = rope_tables(positions, HEAD)
    causal_mask = positions[:, None] >= positions[None, :]
    stacked = (norm_attn, w_q, w_kv, w_o, norm_mlp, w_gate, w_up, w_down)

    def one_sequence(seq_tokens):
        def layer_step(resid, layer_w):
            return decoder_layer(resid, layer_w, cos_t, sin_t, causal_mask), None
        final, _ = lax.scan(layer_step, seq_tokens.astype(jnp.float32), stacked)
        return final.astype(jnp.bfloat16)

    return lax.map(one_sequence, hidden)
```

```python
import functools
import math
import jax
import jax.numpy as jnp
from jax import lax
from jax.experimental import pallas as pl
from jax.experimental.pallas import tpu as pltpu
from jax.sharding import PartitionSpec as P

EPS = 1e-5
ROPE_BASE = 10000.0
MESH = pl.DeviceIdType.MESH
NZ = 4
LANES = 128


class Cfg:
    def __init__(self, layers, seq, width, heads, head, ff):
        self.L, self.S, self.D, self.H, self.E, self.F = layers, seq, width, heads, head, ff
        self.T = seq // 8
        self.CK = 512
        self.NK = width // self.CK
        self.CN = 512
        self.NN = width // self.CN
        self.NG = 5
        self.ND = 4
        self.NR = 3
        self.SUB = 128
        self.AHEAD = 3


def kernel(cfg, hid_ref, na_ref, nm_ref, cos_ref, sin_ref, mask_ref,
           wq_hbm, wkv_hbm, wo_hbm, wg_hbm, wu_hbm, wd_hbm, out_ref,
           xg, rsd, rsb, stg_d, stg_o, qb, resid, wqkv, raw, scr, wo_b, gu_b, wd_b,
           qkv, gacc, uacc, act, ctx,
           s_wq, s_kv, s_wo, s_gu, s_wd,
           r_dir, r_par, s_own, s_far, s_par,
           q_par, q_dir, t_par, t_dir):
    c = cfg
    L, S, D, H, E, T = c.L, c.S, c.D, c.H, c.E, c.T
    HS = S // 2
    dp = lax.axis_index("dp")
    tp = lax.axis_index("tp")
    z = tp // 2
    core = lax.rem(tp, 2)
    partner = tp + 1 - 2 * core
    middle = jnp.logical_or(z == 1, z == 2)
    far = jnp.where(z == 1, 3, 0)
    near = jnp.where(z == 1, 0, 3)

    def chip(zz):
        return 2 * zz + core

    def rcopy(src, dst, ss, rs, to):
        return pltpu.make_async_remote_copy(src_ref=src, dst_ref=dst, send_sem=ss, recv_sem=rs,
                                            device_id=(dp, to), device_id_type=MESH)

    def blk(zz, base=0):
        return pl.ds(pl.multiple_of(base + zz * T, T), T)

    def kcols(k):
        return pl.ds(pl.multiple_of(k * c.CK, c.CK), c.CK)

    def ncols(j):
        return pl.ds(pl.multiple_of(j * c.CN, c.CN), c.CN)

    def wq_copy(l, h):
        return pltpu.make_async_copy(wq_hbm.at[l, h], wqkv.at[:, pl.ds(h * E, E)], s_wq.at[h])

    pair = pl.multiple_of(2 * (tp // 2), 2)

    def kv_copy(g):
        l, k, slot = g // c.NK, lax.rem(g, c.NK), lax.rem(g, c.NR)
        return pltpu.make_async_copy(
            wkv_hbm.at[l, pl.ds(pl.multiple_of(k * c.CK, c.CK), c.CK), :, pl.ds(pair, 2)],
            raw.at[slot], s_kv.at[slot])

    def wo_copy(l):
        return pltpu.make_async_copy(wo_hbm.at[l], wo_b, s_wo)

    def gu_copies(g):
        l, k, slot = g // c.NK, lax.rem(g, c.NK), lax.rem(g, c.NG)
        return [pltpu.make_async_copy(w.at[l, :, kcols(k)], gu_b.at[slot, i], s_gu.at[slot, i])
                for i, w in enumerate((wg_hbm, wu_hbm))]

    def wd_copy(g):
        l, j, slot = g // c.NN, lax.rem(g, c.NN), lax.rem(g, c.ND)
        return pltpu.make_async_copy(wd_hbm.at[l, :, ncols(j)], wd_b.at[slot], s_wd.at[slot])

    for h in range(H):
        wq_copy(0, h).start()
    for g in range(c.NR):
        kv_copy(g).start()

    bar = pltpu.get_barrier_semaphore()
    pl.semaphore_signal(bar, inc=1, device_id=(dp, partner), device_id_type=MESH)
    for d in range(1, NZ):
        pl.semaphore_signal(bar, inc=1, device_id=(dp, chip(lax.rem(z + d, NZ))), device_id_type=MESH)
    pl.semaphore_wait(bar, NZ)

    def gather_phase(l, ph, compute):
        buf = xg.at[l, ph]

        def own(k):
            src = buf.at[blk(z), kcols(k)]
            res = [(None, rcopy(src, buf.at[blk(z, HS), kcols(k)], s_own.at[0, k], r_par.at[l, ph, z, k], partner))]
            for i, dz in enumerate((2, -2, 1, -1)):
                ok = jnp.logical_and(z + dz >= 0, z + dz < NZ)
                to = chip(jnp.clip(z + dz, 0, NZ - 1))
                res.append((ok, rcopy(src, src, s_own.at[1 + i, k], r_dir.at[l, ph, z, k], to)))
            return res

        def dir_in(o, k):
            b = buf.at[blk(o), kcols(k)]
            return rcopy(b, b, s_far.at[k], r_dir.at[l, ph, o, k], partner)

        def far_send(k):
            b = buf.at[blk(far), kcols(k)]
            return rcopy(b, b, s_far.at[k], r_dir.at[l, ph, far, k], chip(near))

        def par_send(o, k):
            return rcopy(buf.at[blk(o), kcols(k)], buf.at[blk(o, HS), kcols(k)],
                         s_par.at[o, k], r_par.at[l, ph, o, k], partner)

        def start_own(k):
            for ok, cp in own(k):
                if ok is None:
                    cp.start()
                else:
                    @pl.when(ok)
                    def _(cp=cp):
                        cp.start()

        def stage_far(k):
            @pl.when(middle)
            def _():
                dir_in(far, k).wait_recv()
                far_send(k).start()

        def stage_par(k):
            for o in range(NZ):
                @pl.when(jnp.logical_and(o != z, jnp.logical_not(jnp.logical_and(middle, o == far))))
                def _(o=o):
                    dir_in(o, k).wait_recv()
                    par_send(o, k).start()

                @pl.when(jnp.logical_and(middle, o == far))
                def _(o=o):
                    par_send(o, k).start()

        def stage_in(k):
            for o in range(NZ):
                par_send(o, k).wait_recv()

        for k in range(min(c.AHEAD, c.NK)):
            start_own(k)

        def step(i, _):
            @pl.when(i + c.AHEAD < c.NK)
            def _():
                start_own(i + c.AHEAD)

            @pl.when(i < c.NK)
            def _():
                stage_far(i)

            @pl.when(jnp.logical_and(i >= 1, i < c.NK + 1))
            def _():
                stage_par(i - 1)

            @pl.when(i >= 2)
            def _():
                stage_in(i - 2)
                compute(i - 2)
            return 0

        lax.fori_loop(0, c.NK + 2, step, 0)

        def drain(k, _):
            for ok, cp in own(k):
                if ok is None:
                    cp.wait_send()
                else:
                    @pl.when(ok)
                    def _(cp=cp):
                        cp.wait_send()

            @pl.when(middle)
            def _():
                far_send(k).wait_send()
            for o in range(NZ):
                @pl.when(o != z)
                def _(o=o):
                    par_send(o, k).wait_send()
            return 0

        lax.fori_loop(0, c.NK, drain, 0)

    def reduce_phase(l, ph, produce):
        def par(j):
            return rcopy(stg_d.at[:, ncols(j)], rsd.at[l, ph, :, ncols(j)], t_par.at[j], q_par.at[l, ph, j], partner)

        def out(d, j):
            is_far = (z == 0) if d == 3 else (z == 3)
            if d in (0, 3):
                mid = 1 if d == 3 else 2
                to = jnp.where(is_far, mid, d)
                slot = jnp.where(is_far, mid, z)
                ok = jnp.logical_or(z == 0, z == 2) if d == 3 else jnp.logical_or(z == 1, z == 3)
            else:
                to, slot, ok = d, z, z != d
            return ok, rcopy(stg_o.at[blk(d), ncols(j)], rsb.at[l, ph, slot, :, ncols(j)],
                             t_dir.at[d, j], q_dir.at[l, ph, slot, j], chip(to))

        def mid_send(j):
            return rcopy(stg_o.at[blk(far), ncols(j)], rsb.at[l, ph, z, :, ncols(j)],
                         t_dir.at[far, j], q_dir.at[l, ph, z, j], chip(far))

        def dir_in(slot, j):
            b = rsb.at[l, ph, slot, :, ncols(j)]
            return rcopy(b, b, t_dir.at[0, j], q_dir.at[l, ph, slot, j], partner)

        def stage_make(j):
            part = produce(j)
            qb[:, ncols(j)] = part[:HS]
            stg_d[:, ncols(j)] = part[HS:].astype(jnp.bfloat16)
            par(j).start()

        def stage_pair(j):
            par(j).wait_recv()
            both = qb[:, ncols(j)] + rsd[l, ph, :, ncols(j)].astype(jnp.float32)
            qb[:, ncols(j)] = both
            stg_o[:, ncols(j)] = both.astype(jnp.bfloat16)
            for d in (3, 0, 2, 1):
                ok, cp = out(d, j)

                @pl.when(ok)
                def _(cp=cp):
                    cp.start()

        def stage_mid(j):
            @pl.when(middle)
            def _():
                dir_in(z, j).wait_recv()
                both = qb[blk(far), ncols(j)] + rsb[l, ph, z, :, ncols(j)].astype(jnp.float32)
                stg_o[blk(far), ncols(j)] = both.astype(jnp.bfloat16)
                mid_send(j).start()

        def stage_sum(j):
            resid[:, ncols(j)] = resid[:, ncols(j)] + qb[blk(z), ncols(j)]
            for s in range(NZ):
                dist = jnp.abs(z - s)

                @pl.when(jnp.logical_and(dist >= 1, dist <= 2))
                def _(s=s):
                    dir_in(s, j).wait_recv()
                    resid[:, ncols(j)] = resid[:, ncols(j)] + rsb[l, ph, s, :, ncols(j)].astype(jnp.float32)

        def step(i, _):
            @pl.when(i < c.NN)
            def _():
                stage_make(i)

            @pl.when(jnp.logical_and(i >= 1, i < c.NN + 1))
            def _():
                stage_pair(i - 1)

            @pl.when(jnp.logical_and(i >= 2, i < c.NN + 2))
            def _():
                stage_mid(i - 2)

            @pl.when(i >= 4)
            def _():
                stage_sum(i - 4)
            return 0

        lax.fori_loop(0, c.NN + 4, step, 0)

        def drain(j, _):
            par(j).wait_send()
            for d in range(NZ):
                ok, cp = out(d, j)

                @pl.when(ok)
                def _(cp=cp):
                    cp.wait_send()

            @pl.when(middle)
            def _():
                mid_send(j).wait_send()
            return 0

        lax.fori_loop(0, c.NN, drain, 0)

    def norm_into(l, ph, gain_ref):
        r = resid[...]
        inv = lax.rsqrt(jnp.mean(r * r, axis=-1, keepdims=True) + EPS)
        xg[l, ph, blk(z), :] = (r * inv * gain_ref[l]).astype(jnp.bfloat16)

    def rope(x):
        return x * cos_ref[...] + pltpu.roll(x, E // 2, 1) * sin_ref[...]

    def attention():
        inv_sqrt = 1.0 / math.sqrt(E)
        keys = rope(qkv[:, H * E:(H + 1) * E]).astype(jnp.bfloat16)
        values = qkv[:, (H + 1) * E:].astype(jnp.bfloat16)
        keep = mask_ref[...] > 0.5
        for h in range(H):
            q = rope(qkv[:, h * E:(h + 1) * E]).astype(jnp.bfloat16)
            s = lax.dot_general(q, keys, (((1,), (1,)), ((), ())), preferred_element_type=jnp.float32) * inv_sqrt
            s = jnp.where(keep, s, -jnp.inf)
            e = jnp.exp(s - jnp.max(s, axis=-1, keepdims=True))
            p = (e / jnp.sum(e, axis=-1, keepdims=True)).astype(jnp.bfloat16)
            ctx[:, h * E:(h + 1) * E] = jnp.dot(p, values, preferred_element_type=jnp.float32).astype(jnp.bfloat16)

    resid[...] = hid_ref[...].astype(jnp.float32)
    par_head = lax.rem(tp, 2)

    def layer(l, _):
        norm_into(l, 0, na_ref)

        def qkv_chunk(k):
            @pl.when(k == 0)
            def _():
                for h in range(H):
                    wq_copy(l, h).wait()
                qkv[...] = jnp.zeros_like(qkv)

            @pl.when(jnp.logical_and(l == 0, k == 0))
            def _():
                wo_copy(0).start()
            for n in range(c.NG):
                @pl.when(jnp.logical_and(l == 0, k == 1 + n))
                def _(n=n):
                    for cp in gu_copies(n):
                        cp.start()
            for n in range(c.ND):
                @pl.when(jnp.logical_and(l == 0, k == 1 + c.NG + n))
                def _(n=n):
                    wd_copy(n).start()
            g = l * c.NK + k
            kv_copy(g).wait()
            slot = lax.rem(g, c.NR)

            def sub(s, _):
                r0 = pl.multiple_of(s * c.SUB, c.SUB)
                scr[...] = raw[slot, pl.ds(r0, c.SUB)].astype(jnp.float32).reshape(c.SUB * 4, LANES)
                for i in range(2):
                    y = scr[pl.ds(2 * i + par_head, c.SUB, stride=4), :]
                    wqkv[pl.ds(pl.multiple_of(k * c.CK + r0, c.SUB), c.SUB),
                         (H + i) * E:(H + 1 + i) * E] = y.astype(jnp.bfloat16)
                return 0

            lax.fori_loop(0, c.CK // c.SUB, sub, 0)

            @pl.when(g + c.NR < L * c.NK)
            def _():
                kv_copy(g + c.NR).start()
            rows = pl.ds(pl.multiple_of(k * c.CK, c.CK), c.CK)
            qkv[...] += jnp.dot(xg[l, 0, :, kcols(k)], wqkv[rows, :], preferred_element_type=jnp.float32)

        gather_phase(l, 0, qkv_chunk)

        @pl.when(l + 1 < L)
        def _():
            for h in range(H):
                wq_copy(l + 1, h).start()
        attention()
        wo_copy(l).wait()
        reduce_phase(l, 0, lambda j: jnp.dot(ctx[...], wo_b[:, ncols(j)], preferred_element_type=jnp.float32))

        @pl.when(l + 1 < L)
        def _():
            wo_copy(l + 1).start()
        norm_into(l, 1, nm_ref)

        def gu_chunk(k):
            @pl.when(k == 0)
            def _():
                gacc[...] = jnp.zeros_like(gacc)
                uacc[...] = jnp.zeros_like(uacc)
            g = l * c.NK + k
            slot = lax.rem(g, c.NG)
            x = xg[l, 1, :, kcols(k)]
            for i, (cp, acc) in enumerate(zip(gu_copies(g), (gacc, uacc))):
                cp.wait()
                acc[...] += lax.dot_general(x, gu_b[slot, i], (((1,), (1,)), ((), ())),
                                            preferred_element_type=jnp.float32)

            @pl.when(g + c.NG < L * c.NK)
            def _():
                for cp in gu_copies(g + c.NG):
                    cp.start()

        gather_phase(l, 1, gu_chunk)
        gate = gacc[...]
        act[...] = (gate * jax.nn.sigmoid(gate) * uacc[...]).astype(jnp.bfloat16)

        def down_chunk(j):
            g = l * c.NN + j
            slot = lax.rem(g, c.ND)
            wd_copy(g).wait()
            part = jnp.dot(act[...], wd_b[slot], preferred_element_type=jnp.float32)

            @pl.when(g + c.ND < L * c.NN)
            def _():
                wd_copy(g + c.ND).start()
            return part

        reduce_phase(l, 1, down_chunk)
        return 0

    lax.fori_loop(0, L, layer, 0)
    out_ref[...] = resid[...].astype(jnp.bfloat16)


def solution(mesh):
    tok_spec = P('dp', 'tp', None)
    in_specs = (tok_spec, P(), P(None, None, 'tp', None), P(), P(None, 'tp', None, None), P(), P(None, None, 'tp'), P(None, None, 'tp'), P(None, 'tp', None))

    def body(hidden, norm_attn, w_q, w_kv, w_o, norm_mlp, w_gate, w_up, w_down):
        L, D, H, E = w_q.shape
        F = w_gate.shape[2]
        T = hidden.shape[1]
        S = 8 * T
        cfg = Cfg(L, S, D, H, E, F)
        core = lax.rem(lax.axis_index('tp'), 2)
        row = jnp.arange(S)
        cls = jnp.where(row < S // 2, core, 1 - core)
        pos = ((row % (S // 2)) // T) * (2 * T) + cls * T + row % T
        inv_freq = jnp.power(ROPE_BASE, -2.0 * jnp.arange(E // 2, dtype=jnp.float32) / E)
        ang = pos.astype(jnp.float32)[:, None] * inv_freq[None, :]
        cos_t, sin_t = jnp.cos(ang), jnp.sin(ang)
        cos_f = jnp.concatenate([cos_t, cos_t], axis=1)
        sin_f = jnp.concatenate([-sin_t, sin_t], axis=1)
        mask = (pos[:, None] >= pos[None, :]).astype(jnp.float32)

        c = cfg
        bf, f32 = jnp.bfloat16, jnp.float32
        vm = pl.BlockSpec(memory_space=pltpu.VMEM)
        hb = pl.BlockSpec(memory_space=pl.ANY)
        dma = pltpu.SemaphoreType.DMA
        scratch = [
            pltpu.VMEM((L, 2, S, D), bf),
            pltpu.VMEM((L, 2, S // 2, D), bf),
            pltpu.VMEM((L, 2, NZ, T, D), bf),
            pltpu.VMEM((S // 2, D), bf),
            pltpu.VMEM((S // 2, D), bf),
            pltpu.VMEM((S // 2, D), f32),
            pltpu.VMEM((T, D), f32),
            pltpu.VMEM((D, (H + 2) * E), bf),
            pltpu.VMEM((c.NR, c.CK, 2, 2, E), bf),
            pltpu.VMEM((c.SUB * 4, E), f32),
            pltpu.VMEM((H * E, D), bf),
            pltpu.VMEM((c.NG, 2, F, c.CK), bf),
            pltpu.VMEM((c.ND, F, c.CN), bf),
            pltpu.VMEM((S, (H + 2) * E), f32),
            pltpu.VMEM((S, F), f32),
            pltpu.VMEM((S, F), f32),
            pltpu.VMEM((S, F), bf),
            pltpu.VMEM((S, H * E), bf),
            dma((H,)), dma((c.NR,)), dma, dma((c.NG, 2)), dma((c.ND,)),
            dma((L, 2, NZ, c.NK)), dma((L, 2, NZ, c.NK)), dma((5, c.NK)), dma((c.NK,)), dma((NZ, c.NK)),
            dma((L, 2, c.NN)), dma((L, 2, NZ, c.NN)), dma((c.NN,)), dma((NZ, c.NN)),
        ]
        out = pl.pallas_call(
            functools.partial(kernel, cfg),
            out_shape=jax.ShapeDtypeStruct((T, D), bf),
            in_specs=[vm] * 6 + [hb] * 6,
            out_specs=vm,
            scratch_shapes=scratch,
            compiler_params=pltpu.CompilerParams(collective_id=0, has_side_effects=True, vmem_limit_bytes=67043328),
            name="layers",
        )(hidden[0], norm_attn.reshape(L, 1, D), norm_mlp.reshape(L, 1, D), cos_f, sin_f, mask,
          jnp.transpose(w_q, (0, 2, 1, 3)), w_kv, w_o.reshape(L, H * E, D),
          jnp.transpose(w_gate, (0, 2, 1)), jnp.transpose(w_up, (0, 2, 1)), w_down)
        return out[None]

    return jax.shard_map(body, mesh=mesh, in_specs=in_specs, out_specs=tok_spec, check_vma=False)
```

```python
import functools
import math
import jax
import jax.numpy as jnp
from jax import lax
from jax.experimental import pallas as pl
from jax.experimental.pallas import tpu as pltpu
from jax.sharding import PartitionSpec as P

EPS = 1e-5
ROPE_BASE = 10000.0
MESH = pl.DeviceIdType.MESH
NZ = 4
LANES = 128


class Cfg:
    def __init__(self, layers, seq, width, heads, head, ff):
        self.L, self.S, self.D, self.H, self.E, self.F = layers, seq, width, heads, head, ff
        self.T = seq // 8
        self.CKS = (1280, 1024)
        self.NKS = tuple(width // n for n in self.CKS)
        self.KC = 512
        self.NC = width // self.KC
        self.FP = -(-ff // LANES) * LANES
        self.CN = 1024
        self.NN = width // self.CN
        self.NG = 2
        self.ND = 2
        self.NR = 3
        self.SUB = 128
        self.AHEAD = (4, 3)
        self.LF, self.LP, self.LC = 0, 1, 2
        self.RP, self.RA, self.RB, self.RM, self.RS = 2, 3, 4, 4, 6


def kernel(cfg, hid_hbm, na_hbm, nm_hbm, wq_hbm, wkv_hbm, wo_hbm, wg_hbm, wu_hbm, wd_hbm, out_ref,
           xg, rsd, rsb, stg_d, stg_o, qb, resid, wqkv, raw, scr, wo_b, gu_b, wd_b,
           qkv, gacc, act, ctx, hid_ref, na_ref, nm_ref, cos_ref, sin_ref, mask_ref, s_in,
           s_wq, s_kv, s_wo, s_gu, s_wd,
           r_dir, r_par, s_own, s_far, s_near, s_par,
           q_par, q_dir, t_par, t_dir):
    c = cfg
    L, S, D, H, E, T = c.L, c.S, c.D, c.H, c.E, c.T
    HS = S // 2
    dp = lax.axis_index("dp")
    tp = lax.axis_index("tp")
    z = tp // 2
    core = lax.rem(tp, 2)
    partner = tp + 1 - 2 * core
    middle = jnp.logical_or(z == 1, z == 2)
    far = jnp.where(z == 1, 3, 0)
    near = jnp.where(z == 1, 0, 3)

    def chip(zz):
        return 2 * zz + core

    def rcopy(src, dst, ss, rs, to):
        return pltpu.make_async_remote_copy(src_ref=src, dst_ref=dst, send_sem=ss, recv_sem=rs,
                                            device_id=(dp, to), device_id_type=MESH)

    def blk(zz, base=0):
        return pl.ds(pl.multiple_of(base + zz * T, T), T)

    def kcols(ph, k):
        return pl.ds(pl.multiple_of(k * c.CKS[ph], c.CKS[ph]), c.CKS[ph])

    def ncols(j):
        return pl.ds(pl.multiple_of(j * c.CN, c.CN), c.CN)

    def wq_copy(l, h):
        return pltpu.make_async_copy(wq_hbm.at[l, h], wqkv.at[:, pl.ds(h * E, E)], s_wq.at[h])

    pair = pl.multiple_of(2 * (tp // 2), 2)

    def kv_copy(g):
        l, k, slot = g // c.NC, lax.rem(g, c.NC), lax.rem(g, c.NR)
        return pltpu.make_async_copy(
            wkv_hbm.at[l, pl.ds(pl.multiple_of(k * c.KC, c.KC), c.KC), :, pl.ds(pair, 2)],
            raw.at[slot], s_kv.at[slot])

    def wo_copy(l):
        return pltpu.make_async_copy(wo_hbm.at[l], wo_b, s_wo)

    def gu_copies(g):
        l, k, slot = g // c.NKS[1], lax.rem(g, c.NKS[1]), lax.rem(g, c.NG)
        return [pltpu.make_async_copy(w.at[l, :, kcols(1, k)], gu_b.at[slot, pl.ds(i * c.FP, c.F)], s_gu.at[slot, i])
                for i, w in enumerate((wg_hbm, wu_hbm))]

    def wd_copy(g):
        l, j, slot = g // c.NN, lax.rem(g, c.NN), lax.rem(g, c.ND)
        return pltpu.make_async_copy(wd_hbm.at[l, :, ncols(j)], wd_b.at[slot], s_wd.at[slot])

    bar = pltpu.get_barrier_semaphore()
    pl.semaphore_signal(bar, inc=1, device_id=(dp, partner), device_id_type=MESH)
    for d in range(1, NZ):
        pl.semaphore_signal(bar, inc=1, device_id=(dp, chip(lax.rem(z + d, NZ))), device_id_type=MESH)

    inputs = [pltpu.make_async_copy(a, b, s_in.at[i])
              for i, (a, b) in enumerate(((hid_hbm, hid_ref), (na_hbm, na_ref), (nm_hbm, nm_ref)))]
    for cp in inputs:
        cp.start()
    for g in range(c.NR):
        kv_copy(g).start()
    for h in range(H):
        wq_copy(0, h).start()

    def gather_phase(l, ph, compute, before=None):
        buf = xg.at[l, ph]
        nk = c.NKS[ph]

        def own(k):
            src = buf.at[blk(z), kcols(ph, k)]
            res = [(None, rcopy(src, buf.at[blk(z, HS), kcols(ph, k)], s_own.at[0, k], r_par.at[l, ph, z, k], partner))]
            for i, dz in enumerate((2, -2, 1, -1)):
                ok = jnp.logical_and(z + dz >= 0, z + dz < NZ)
                if abs(dz) == 1:
                    late = jnp.logical_and(middle, z + dz == near)
                    ok = jnp.logical_and(ok, jnp.logical_not(late))
                to = chip(jnp.clip(z + dz, 0, NZ - 1))
                res.append((ok, rcopy(src, src, s_own.at[1 + i, k], r_dir.at[l, ph, z, k], to)))
            return res

        def near_send(k):
            b = buf.at[blk(z), kcols(ph, k)]
            return rcopy(b, b, s_near.at[k], r_dir.at[l, ph, z, k], chip(near))

        def dir_in(o, k):
            b = buf.at[blk(o), kcols(ph, k)]
            return rcopy(b, b, s_far.at[k], r_dir.at[l, ph, o, k], partner)

        def far_send(k):
            b = buf.at[blk(far), kcols(ph, k)]
            return rcopy(b, b, s_far.at[k], r_dir.at[l, ph, far, k], chip(near))

        def par_send(o, k):
            return rcopy(buf.at[blk(o), kcols(ph, k)], buf.at[blk(o, HS), kcols(ph, k)],
                         s_par.at[o, k], r_par.at[l, ph, o, k], partner)

        def start_own(k):
            for ok, cp in own(k):
                if ok is None:
                    cp.start()
                else:
                    @pl.when(ok)
                    def _(cp=cp):
                        cp.start()

        def stage_far(k):
            @pl.when(middle)
            def _():
                dir_in(far, k).wait_recv()
                far_send(k).start()
                near_send(k).start()

        def stage_par(k):
            for o in range(NZ):
                @pl.when(jnp.logical_and(o != z, jnp.logical_not(jnp.logical_and(middle, o == far))))
                def _(o=o):
                    dir_in(o, k).wait_recv()
                    par_send(o, k).start()

                @pl.when(jnp.logical_and(middle, o == far))
                def _(o=o):
                    par_send(o, k).start()

        def stage_in(k):
            for o in range(NZ):
                par_send(o, k).wait_recv()

        ahead = min(c.AHEAD[ph], nk)
        for k in range(ahead):
            start_own(k)

        if before is not None:
            before()

        def step(i, _):
            if ahead < nk:
                @pl.when(i + ahead < nk)
                def _():
                    start_own(i + ahead)

            @pl.when(jnp.logical_and(i >= c.LF, i < nk + c.LF))
            def _():
                stage_far(i - c.LF)

            @pl.when(jnp.logical_and(i >= c.LP, i < nk + c.LP))
            def _():
                stage_par(i - c.LP)

            @pl.when(i >= c.LC)
            def _():
                stage_in(i - c.LC)
                compute(i - c.LC)
            return 0

        lax.fori_loop(0, nk + c.LC, step, 0)

        def drain(k, _):
            for ok, cp in own(k):
                if ok is None:
                    cp.wait_send()
                else:
                    @pl.when(ok)
                    def _(cp=cp):
                        cp.wait_send()

            @pl.when(middle)
            def _():
                far_send(k).wait_send()
                near_send(k).wait_send()
            for o in range(NZ):
                @pl.when(o != z)
                def _(o=o):
                    par_send(o, k).wait_send()
            return 0

        lax.fori_loop(0, nk, drain, 0)

    def reduce_phase(l, ph, produce, beside=None):
        def par(j):
            return rcopy(stg_d.at[:, ncols(j)], rsd.at[l, ph, :, ncols(j)], t_par.at[j], q_par.at[l, ph, j], partner)

        def out(d, j):
            is_far = (z == 0) if d == 3 else (z == 3)
            if d in (0, 3):
                mid = 1 if d == 3 else 2
                to = jnp.where(is_far, mid, d)
                slot = jnp.where(is_far, mid, z)
                ok = jnp.logical_or(z == 0, z == 2) if d == 3 else jnp.logical_or(z == 1, z == 3)
            else:
                to, slot, ok = d, z, z != d
            return ok, rcopy(stg_o.at[blk(d), ncols(j)], rsb.at[l, ph, slot, :, ncols(j)],
                             t_dir.at[d, j], q_dir.at[l, ph, slot, j], chip(to))

        def mid_send(j):
            return rcopy(stg_o.at[blk(far), ncols(j)], rsb.at[l, ph, z, :, ncols(j)],
                         t_dir.at[far, j], q_dir.at[l, ph, z, j], chip(far))

        def dir_in(slot, j):
            b = rsb.at[l, ph, slot, :, ncols(j)]
            return rcopy(b, b, t_dir.at[0, j], q_dir.at[l, ph, slot, j], partner)

        def stage_make(j):
            part = produce(j)
            qb[:, ncols(j)] = part[:HS]
            stg_d[:, ncols(j)] = part[HS:].astype(jnp.bfloat16)
            par(j).start()

        def send(j, order, which):
            for d in order:
                ok, cp = out(d, j)

                @pl.when(jnp.logical_and(ok, which(d)))
                def _(cp=cp):
                    cp.start()

        def stage_pair(j):
            par(j).wait_recv()
            both = qb[:, ncols(j)] + rsd[l, ph, :, ncols(j)].astype(jnp.float32)
            qb[:, ncols(j)] = both
            stg_o[:, ncols(j)] = both.astype(jnp.bfloat16)
            send(j, (3, 0, 2, 1), lambda d: jnp.logical_or(middle, z == 3 - d) if d in (0, 3) else middle)

        def stage_mid(j):
            @pl.when(middle)
            def _():
                dir_in(z, j).wait_recv()
                both = qb[blk(far), ncols(j)] + rsb[l, ph, z, :, ncols(j)].astype(jnp.float32)
                stg_o[blk(far), ncols(j)] = both.astype(jnp.bfloat16)
                mid_send(j).start()

        def stage_sum(j):
            resid[:, ncols(j)] = resid[:, ncols(j)] + qb[blk(z), ncols(j)]
            for s in range(NZ):
                dist = jnp.abs(z - s)

                @pl.when(jnp.logical_and(dist >= 1, dist <= 2))
                def _(s=s):
                    dir_in(s, j).wait_recv()
                    resid[:, ncols(j)] = resid[:, ncols(j)] + rsb[l, ph, s, :, ncols(j)].astype(jnp.float32)

        def step(i, _):
            @pl.when(i < c.NN)
            def _():
                stage_make(i)

            @pl.when(jnp.logical_and(i >= c.RP, i < c.NN + c.RP))
            def _():
                stage_pair(i - c.RP)

            if beside is not None:
                beside(i)

            @pl.when(jnp.logical_and(i >= c.RA, i < c.NN + c.RA))
            def _():
                send(i - c.RA, (2, 1), lambda d: z == (0 if d == 2 else 3))

            @pl.when(jnp.logical_and(i >= c.RB, i < c.NN + c.RB))
            def _():
                send(i - c.RB, (1, 2), lambda d: z == (0 if d == 1 else 3))

            @pl.when(jnp.logical_and(i >= c.RM, i < c.NN + c.RM))
            def _():
                stage_mid(i - c.RM)

            @pl.when(i >= c.RS)
            def _():
                stage_sum(i - c.RS)
            return 0

        lax.fori_loop(0, c.NN + c.RS, step, 0)

        def drain(j, _):
            par(j).wait_send()
            for d in range(NZ):
                ok, cp = out(d, j)

                @pl.when(ok)
                def _(cp=cp):
                    cp.wait_send()

            @pl.when(middle)
            def _():
                mid_send(j).wait_send()
            return 0

        lax.fori_loop(0, c.NN, drain, 0)

    def norm_into(l, ph, gain_ref):
        r = resid[...]
        inv = lax.rsqrt(jnp.mean(r * r, axis=-1, keepdims=True) + EPS)
        xg[l, ph, blk(z), :] = (r * inv * gain_ref[pl.ds(l, 1), :]).astype(jnp.bfloat16)

    def rope(x):
        return x * cos_ref[...] + pltpu.roll(x, E // 2, 1) * sin_ref[...]

    def attention():
        inv_sqrt = 1.0 / math.sqrt(E)
        keys = rope(qkv[:, H * E:(H + 1) * E]).astype(jnp.bfloat16)
        values = qkv[:, (H + 1) * E:].astype(jnp.bfloat16)
        keep = mask_ref[...] > 0.5
        for h in range(H):
            q = rope(qkv[:, h * E:(h + 1) * E]).astype(jnp.bfloat16)
            s = lax.dot_general(q, keys, (((1,), (1,)), ((), ())), preferred_element_type=jnp.float32) * inv_sqrt
            s = jnp.where(keep, s, -jnp.inf)
            e = jnp.exp(s - jnp.max(s, axis=-1, keepdims=True))
            p = (e / jnp.sum(e, axis=-1, keepdims=True)).astype(jnp.bfloat16)
            ctx[:, h * E:(h + 1) * E] = jnp.dot(p, values, preferred_element_type=jnp.float32).astype(jnp.bfloat16)

    par_head = lax.rem(tp, 2)

    def kv_take(l, k):
        g = l * c.NC + k
        kv_copy(g).wait()
        slot = lax.rem(g, c.NR)

        def sub(s, _):
            r0 = pl.multiple_of(s * c.SUB, c.SUB)
            scr[...] = raw[slot, pl.ds(r0, c.SUB)].astype(jnp.float32).reshape(c.SUB * 4, LANES)
            for i in range(2):
                y = scr[pl.ds(2 * i + par_head, c.SUB, stride=4), :]
                wqkv[pl.ds(pl.multiple_of(k * c.KC + r0, c.SUB), c.SUB),
                     (H + i) * E:(H + 1 + i) * E] = y.astype(jnp.bfloat16)
            return 0

        lax.fori_loop(0, c.KC // c.SUB, sub, 0)

        @pl.when(g + c.NR < L * c.NC)
        def _():
            kv_copy(g + c.NR).start()

    def tables():
        def position(row):
            cls = jnp.where(row < HS, core, 1 - core)
            return (lax.shift_right_logical(row & (HS - 1), T.bit_length() - 1) * (2 * T)
                    + cls * T + (row & (T - 1)))

        pos = position(lax.broadcasted_iota(jnp.int32, (S, E), 0))
        lane = lax.broadcasted_iota(jnp.int32, (S, E), 1)
        pair_i = (lane & (E // 2 - 1)).astype(jnp.float32)
        ang = pos.astype(jnp.float32) * jnp.exp(pair_i * (-2.0 * math.log(ROPE_BASE) / E))
        cos_ref[...] = jnp.cos(ang)
        sin = jnp.sin(ang)
        sin_ref[...] = jnp.where(lane < E // 2, -sin, sin)
        kpos = position(lax.broadcasted_iota(jnp.int32, (S, S), 1))
        qpos = position(lax.broadcasted_iota(jnp.int32, (S, S), 0))
        mask_ref[...] = jnp.where(qpos >= kpos, 1.0, 0.0)

    gu_b[:, c.F:c.FP, :] = jnp.zeros((c.NG, c.FP - c.F, c.CKS[1]), jnp.bfloat16)
    for cp in inputs:
        cp.wait()
    resid[...] = hid_ref[...].astype(jnp.float32)
    norm_into(0, 0, na_ref)
    pl.semaphore_wait(bar, NZ)

    def layer(l, _):
        @pl.when(l > 0)
        def _():
            norm_into(l, 0, na_ref)

        def qkv_chunk(k):
            @pl.when(k == 0)
            def _():
                for h in range(H):
                    wq_copy(l, h).wait()
                qkv[...] = jnp.zeros_like(qkv)

            @pl.when(jnp.logical_and(l == 0, k == 0))
            def _():
                for n in range(c.NG):
                    for cp in gu_copies(n):
                        cp.start()
                for n in range(c.ND):
                    wd_copy(n).start()
            rows = pl.ds(pl.multiple_of(k * c.CKS[0], c.CKS[0]), c.CKS[0])
            qkv[...] += jnp.dot(xg[l, 0, :, kcols(0, k)], wqkv[rows, :], preferred_element_type=jnp.float32)

        def before():
            @pl.when(l == 0)
            def _():
                tables()
                lax.fori_loop(0, c.NC, lambda k, _: (kv_take(0, k), 0)[1], 0)
                wo_copy(0).start()

        gather_phase(l, 0, qkv_chunk, before)

        @pl.when(l + 1 < L)
        def _():
            for h in range(H):
                wq_copy(l + 1, h).start()
        attention()
        wo_copy(l).wait()

        def take_next(i):
            per = -(-c.NC // c.NN)
            for n in range(per):
                @pl.when(jnp.logical_and(l + 1 < L, i * per + n < c.NC))
                def _(n=n):
                    kv_take(l + 1, i * per + n)

        reduce_phase(l, 0, lambda j: jnp.dot(ctx[...], wo_b[:, ncols(j)], preferred_element_type=jnp.float32),
                     take_next)

        @pl.when(l + 1 < L)
        def _():
            wo_copy(l + 1).start()
        norm_into(l, 1, nm_ref)

        def gu_chunk(k):
            @pl.when(k == 0)
            def _():
                gacc[...] = jnp.zeros_like(gacc)
            g = l * c.NKS[1] + k
            slot = lax.rem(g, c.NG)
            for cp in gu_copies(g):
                cp.wait()
            gacc[...] += lax.dot_general(xg[l, 1, :, kcols(1, k)], gu_b[slot], (((1,), (1,)), ((), ())),
                                         preferred_element_type=jnp.float32)

            @pl.when(g + c.NG < L * c.NKS[1])
            def _():
                for cp in gu_copies(g + c.NG):
                    cp.start()

        gather_phase(l, 1, gu_chunk)
        gate = gacc[:, :c.F]
        act[...] = (gate * jax.nn.sigmoid(gate) * gacc[:, c.FP:c.FP + c.F]).astype(jnp.bfloat16)

        def down_chunk(j):
            g = l * c.NN + j
            slot = lax.rem(g, c.ND)
            wd_copy(g).wait()
            part = jnp.dot(act[...], wd_b[slot], preferred_element_type=jnp.float32)

            @pl.when(g + c.ND < L * c.NN)
            def _():
                wd_copy(g + c.ND).start()
            return part

        reduce_phase(l, 1, down_chunk)
        return 0

    lax.fori_loop(0, L, layer, 0)
    out_ref[...] = resid[...].astype(jnp.bfloat16)


def solution(mesh):
    tok_spec = P('dp', 'tp', None)
    in_specs = (tok_spec, P(), P(None, None, 'tp', None), P(), P(None, 'tp', None, None), P(), P(None, None, 'tp'), P(None, None, 'tp'), P(None, 'tp', None))

    def body(hidden, norm_attn, w_q, w_kv, w_o, norm_mlp, w_gate, w_up, w_down):
        L, D, H, E = w_q.shape
        F = w_gate.shape[2]
        T = hidden.shape[1]
        S = 8 * T
        cfg = Cfg(L, S, D, H, E, F)
        c = cfg
        bf, f32 = jnp.bfloat16, jnp.float32
        vm = pl.BlockSpec(memory_space=pltpu.VMEM)
        hb = pl.BlockSpec(memory_space=pl.ANY)
        dma = pltpu.SemaphoreType.DMA
        mk = max(c.NKS)
        scratch = [
            pltpu.VMEM((L, 2, S, D), bf),
            pltpu.VMEM((L, 2, S // 2, D), bf),
            pltpu.VMEM((L, 2, NZ, T, D), bf),
            pltpu.VMEM((S // 2, D), bf),
            pltpu.VMEM((S // 2, D), bf),
            pltpu.VMEM((S // 2, D), f32),
            pltpu.VMEM((T, D), f32),
            pltpu.VMEM((D, (H + 2) * E), bf),
            pltpu.VMEM((c.NR, c.KC, 2, 2, E), bf),
            pltpu.VMEM((c.SUB * 4, E), f32),
            pltpu.VMEM((H * E, D), bf),
            pltpu.VMEM((c.NG, c.FP + F, c.CKS[1]), bf),
            pltpu.VMEM((c.ND, F, c.CN), bf),
            pltpu.VMEM((S, (H + 2) * E), f32),
            pltpu.VMEM((S, c.FP + F), f32),
            pltpu.VMEM((S, F), bf),
            pltpu.VMEM((S, H * E), bf),
            pltpu.VMEM((T, D), bf), pltpu.VMEM((L, D), f32), pltpu.VMEM((L, D), f32),
            pltpu.VMEM((S, E), f32), pltpu.VMEM((S, E), f32), pltpu.VMEM((S, S), f32),
            dma((3,)),
            dma((H,)), dma((c.NR,)), dma, dma((c.NG, 2)), dma((c.ND,)),
            dma((L, 2, NZ, mk)), dma((L, 2, NZ, mk)), dma((5, mk)), dma((mk,)), dma((mk,)), dma((NZ, mk)),
            dma((L, 2, c.NN)), dma((L, 2, NZ, c.NN)), dma((c.NN,)), dma((NZ, c.NN)),
        ]
        out = pl.pallas_call(
            functools.partial(kernel, cfg),
            out_shape=jax.ShapeDtypeStruct((T, D), bf),
            in_specs=[hb] * 9,
            out_specs=vm,
            scratch_shapes=scratch,
            compiler_params=pltpu.CompilerParams(collective_id=0, has_side_effects=True, vmem_limit_bytes=67043328),
            name="layers",
        )(hidden[0], norm_attn, norm_mlp, jnp.transpose(w_q, (0, 2, 1, 3)), w_kv, w_o.reshape(L, H * E, D),
          jnp.transpose(w_gate, (0, 2, 1)), jnp.transpose(w_up, (0, 2, 1)), w_down)
        return out[None]

    return jax.shard_map(body, mesh=mesh, in_specs=in_specs, out_specs=tok_spec, check_vma=False)
```

```python
import functools
import math
import jax
import jax.numpy as jnp
from jax import lax
from jax.experimental import pallas as pl
from jax.experimental.pallas import tpu as pltpu
from jax.sharding import PartitionSpec as P

EPS = 1e-5
ROPE_BASE = 10000.0
MESH = pl.DeviceIdType.MESH
NZ = 4
LANES = 128


class Cfg:
    def __init__(self, layers, seq, width, heads, head, ff):
        self.L, self.S, self.D, self.H, self.E, self.F = layers, seq, width, heads, head, ff
        self.T = seq // 8
        self.CKS = (1280, 1024)
        self.NKS = tuple(width // n for n in self.CKS)
        self.KC = 512
        self.NC = width // self.KC
        self.CN = 1024
        self.NN = width // self.CN
        self.NG = 2
        self.ND = 4
        self.NR = 3
        self.SUB = 128
        self.AHEAD = (4, 3)
        self.LF, self.LP, self.LC = 0, 1, 2
        self.RP, self.RA, self.RB, self.RM, self.RS = 2, 3, 4, 4, 6


def kernel(cfg, hid_hbm, na_hbm, nm_hbm, wq_hbm, wkv_hbm, wo_hbm, wg_hbm, wu_hbm, wd_hbm, out_ref,
           xg, rsd, rsb, stg_d, stg_o, qb, resid, wqkv, raw, scr, wo_b, gu_b, wd_b,
           qkv, gacc, act, ctx, hid_ref, na_ref, nm_ref, cos_ref, sin_ref, mask_ref, s_in,
           s_wq, s_kv, s_wo, s_gu, s_wd,
           r_dir, r_par, s_own, s_far, s_near, s_par,
           q_par, q_dir, t_par, t_dir):
    c = cfg
    L, S, D, H, E, T = c.L, c.S, c.D, c.H, c.E, c.T
    HS = S // 2
    dp = lax.axis_index("dp")
    tp = lax.axis_index("tp")
    z = tp // 2
    core = lax.rem(tp, 2)
    partner = tp + 1 - 2 * core
    middle = jnp.logical_or(z == 1, z == 2)
    far = jnp.where(z == 1, 3, 0)
    near = jnp.where(z == 1, 0, 3)

    def chip(zz):
        return 2 * zz + core

    def rcopy(src, dst, ss, rs, to):
        return pltpu.make_async_remote_copy(src_ref=src, dst_ref=dst, send_sem=ss, recv_sem=rs,
                                            device_id=(dp, to), device_id_type=MESH)

    def blk(zz, base=0):
        return pl.ds(pl.multiple_of(base + zz * T, T), T)

    def kcols(ph, k):
        return pl.ds(pl.multiple_of(k * c.CKS[ph], c.CKS[ph]), c.CKS[ph])

    def ncols(j):
        return pl.ds(pl.multiple_of(j * c.CN, c.CN), c.CN)

    def wq_copy(l, h):
        return pltpu.make_async_copy(wq_hbm.at[l, h], wqkv.at[:, pl.ds(h * E, E)], s_wq.at[h])

    pair = pl.multiple_of(2 * (tp // 2), 2)

    def kv_copy(g):
        l, k, slot = g // c.NC, lax.rem(g, c.NC), lax.rem(g, c.NR)
        return pltpu.make_async_copy(
            wkv_hbm.at[l, pl.ds(pl.multiple_of(k * c.KC, c.KC), c.KC), :, pl.ds(pair, 2)],
            raw.at[slot], s_kv.at[slot])

    def wo_copy(l):
        return pltpu.make_async_copy(wo_hbm.at[l], wo_b, s_wo)

    def gu_copies(g):
        l, k, slot = g // c.NKS[1], lax.rem(g, c.NKS[1]), lax.rem(g, c.NG)
        return [pltpu.make_async_copy(w.at[l, :, kcols(1, k)], gu_b.at[slot, pl.ds(i * c.F, c.F)], s_gu.at[slot, i])
                for i, w in enumerate((wg_hbm, wu_hbm))]

    def wd_copy(g):
        l, j, slot = g // c.NN, lax.rem(g, c.NN), lax.rem(g, c.ND)
        return pltpu.make_async_copy(wd_hbm.at[l, :, ncols(j)], wd_b.at[slot], s_wd.at[slot])

    bar = pltpu.get_barrier_semaphore()
    pl.semaphore_signal(bar, inc=1, device_id=(dp, partner), device_id_type=MESH)
    for d in range(1, NZ):
        pl.semaphore_signal(bar, inc=1, device_id=(dp, chip(lax.rem(z + d, NZ))), device_id_type=MESH)

    inputs = [pltpu.make_async_copy(a, b, s_in.at[i])
              for i, (a, b) in enumerate(((hid_hbm, hid_ref), (na_hbm, na_ref), (nm_hbm, nm_ref)))]
    for cp in inputs:
        cp.start()
    for g in range(c.NR):
        kv_copy(g).start()
    for h in range(H):
        wq_copy(0, h).start()

    def gather_phase(l, ph, compute, before=None):
        buf = xg.at[l, ph]
        nk = c.NKS[ph]

        def own(k):
            src = buf.at[blk(z), kcols(ph, k)]
            res = [(None, rcopy(src, buf.at[blk(z, HS), kcols(ph, k)], s_own.at[0, k], r_par.at[l, ph, z, k], partner))]
            for i, dz in enumerate((2, -2, 1, -1)):
                ok = jnp.logical_and(z + dz >= 0, z + dz < NZ)
                if abs(dz) == 1:
                    late = jnp.logical_and(middle, z + dz == near)
                    ok = jnp.logical_and(ok, jnp.logical_not(late))
                to = chip(jnp.clip(z + dz, 0, NZ - 1))
                res.append((ok, rcopy(src, src, s_own.at[1 + i, k], r_dir.at[l, ph, z, k], to)))
            return res

        def near_send(k):
            b = buf.at[blk(z), kcols(ph, k)]
            return rcopy(b, b, s_near.at[k], r_dir.at[l, ph, z, k], chip(near))

        def dir_in(o, k):
            b = buf.at[blk(o), kcols(ph, k)]
            return rcopy(b, b, s_far.at[k], r_dir.at[l, ph, o, k], partner)

        def far_send(k):
            b = buf.at[blk(far), kcols(ph, k)]
            return rcopy(b, b, s_far.at[k], r_dir.at[l, ph, far, k], chip(near))

        def par_send(o, k):
            return rcopy(buf.at[blk(o), kcols(ph, k)], buf.at[blk(o, HS), kcols(ph, k)],
                         s_par.at[o, k], r_par.at[l, ph, o, k], partner)

        def start_own(k):
            for ok, cp in own(k):
                if ok is None:
                    cp.start()
                else:
                    @pl.when(ok)
                    def _(cp=cp):
                        cp.start()

        def stage_far(k):
            @pl.when(middle)
            def _():
                dir_in(far, k).wait_recv()
                far_send(k).start()
                near_send(k).start()

        def stage_par(k):
            for o in range(NZ):
                @pl.when(jnp.logical_and(o != z, jnp.logical_not(jnp.logical_and(middle, o == far))))
                def _(o=o):
                    dir_in(o, k).wait_recv()
                    par_send(o, k).start()

                @pl.when(jnp.logical_and(middle, o == far))
                def _(o=o):
                    par_send(o, k).start()

        def stage_in(k):
            for o in range(NZ):
                par_send(o, k).wait_recv()

        ahead = min(c.AHEAD[ph], nk)
        for k in range(ahead):
            start_own(k)

        if before is not None:
            before()

        def step(i, _):
            if ahead < nk:
                @pl.when(i + ahead < nk)
                def _():
                    start_own(i + ahead)

            @pl.when(jnp.logical_and(i >= c.LF, i < nk + c.LF))
            def _():
                stage_far(i - c.LF)

            @pl.when(jnp.logical_and(i >= c.LP, i < nk + c.LP))
            def _():
                stage_par(i - c.LP)

            @pl.when(i >= c.LC)
            def _():
                stage_in(i - c.LC)
                compute(i - c.LC)
            return 0

        lax.fori_loop(0, nk + c.LC, step, 0)

        def drain(k, _):
            for ok, cp in own(k):
                if ok is None:
                    cp.wait_send()
                else:
                    @pl.when(ok)
                    def _(cp=cp):
                        cp.wait_send()

            @pl.when(middle)
            def _():
                far_send(k).wait_send()
                near_send(k).wait_send()
            for o in range(NZ):
                @pl.when(o != z)
                def _(o=o):
                    par_send(o, k).wait_send()
            return 0

        lax.fori_loop(0, nk, drain, 0)

    def reduce_phase(l, ph, produce, beside=None):
        def par(j):
            return rcopy(stg_d.at[:, ncols(j)], rsd.at[l, ph, :, ncols(j)], t_par.at[j], q_par.at[l, ph, j], partner)

        def out(d, j):
            is_far = (z == 0) if d == 3 else (z == 3)
            if d in (0, 3):
                mid = 1 if d == 3 else 2
                to = jnp.where(is_far, mid, d)
                slot = jnp.where(is_far, mid, z)
                ok = jnp.logical_or(z == 0, z == 2) if d == 3 else jnp.logical_or(z == 1, z == 3)
            else:
                to, slot, ok = d, z, z != d
            return ok, rcopy(stg_o.at[blk(d), ncols(j)], rsb.at[l, ph, slot, :, ncols(j)],
                             t_dir.at[d, j], q_dir.at[l, ph, slot, j], chip(to))

        def mid_send(j):
            return rcopy(stg_o.at[blk(far), ncols(j)], rsb.at[l, ph, z, :, ncols(j)],
                         t_dir.at[far, j], q_dir.at[l, ph, z, j], chip(far))

        def dir_in(slot, j):
            b = rsb.at[l, ph, slot, :, ncols(j)]
            return rcopy(b, b, t_dir.at[0, j], q_dir.at[l, ph, slot, j], partner)

        def stage_make(j):
            part = produce(j)
            qb[:, ncols(j)] = part[:HS]
            stg_d[:, ncols(j)] = part[HS:].astype(jnp.bfloat16)
            par(j).start()

        def send(j, order, which):
            for d in order:
                ok, cp = out(d, j)

                @pl.when(jnp.logical_and(ok, which(d)))
                def _(cp=cp):
                    cp.start()

        def stage_pair(j):
            par(j).wait_recv()
            both = qb[:, ncols(j)] + rsd[l, ph, :, ncols(j)].astype(jnp.float32)
            qb[:, ncols(j)] = both
            stg_o[:, ncols(j)] = both.astype(jnp.bfloat16)
            send(j, (3, 0, 2, 1), lambda d: jnp.logical_or(middle, z == 3 - d) if d in (0, 3) else middle)

        def stage_mid(j):
            @pl.when(middle)
            def _():
                dir_in(z, j).wait_recv()
                both = qb[blk(far), ncols(j)] + rsb[l, ph, z, :, ncols(j)].astype(jnp.float32)
                stg_o[blk(far), ncols(j)] = both.astype(jnp.bfloat16)
                mid_send(j).start()

        def stage_sum(j):
            resid[:, ncols(j)] = resid[:, ncols(j)] + qb[blk(z), ncols(j)]
            for s in range(NZ):
                dist = jnp.abs(z - s)

                @pl.when(jnp.logical_and(dist >= 1, dist <= 2))
                def _(s=s):
                    dir_in(s, j).wait_recv()
                    resid[:, ncols(j)] = resid[:, ncols(j)] + rsb[l, ph, s, :, ncols(j)].astype(jnp.float32)

        def step(i, _):
            @pl.when(i < c.NN)
            def _():
                stage_make(i)

            @pl.when(jnp.logical_and(i >= c.RP, i < c.NN + c.RP))
            def _():
                stage_pair(i - c.RP)

            if beside is not None:
                beside(i)

            @pl.when(jnp.logical_and(i >= c.RA, i < c.NN + c.RA))
            def _():
                send(i - c.RA, (2, 1), lambda d: z == (0 if d == 2 else 3))

            @pl.when(jnp.logical_and(i >= c.RB, i < c.NN + c.RB))
            def _():
                send(i - c.RB, (1, 2), lambda d: z == (0 if d == 1 else 3))

            @pl.when(jnp.logical_and(i >= c.RM, i < c.NN + c.RM))
            def _():
                stage_mid(i - c.RM)

            @pl.when(i >= c.RS)
            def _():
                stage_sum(i - c.RS)
            return 0

        lax.fori_loop(0, c.NN + c.RS, step, 0)

        def drain(j, _):
            par(j).wait_send()
            for d in range(NZ):
                ok, cp = out(d, j)

                @pl.when(ok)
                def _(cp=cp):
                    cp.wait_send()

            @pl.when(middle)
            def _():
                mid_send(j).wait_send()
            return 0

        lax.fori_loop(0, c.NN, drain, 0)

    def norm_into(l, ph, gain_ref):
        r = resid[...]
        inv = lax.rsqrt(jnp.mean(r * r, axis=-1, keepdims=True) + EPS)
        xg[l, ph, blk(z), :] = (r * inv * gain_ref[pl.ds(l, 1), :]).astype(jnp.bfloat16)

    def rope(x):
        return x * cos_ref[...] + pltpu.roll(x, E // 2, 1) * sin_ref[...]

    def attention():
        inv_sqrt = 1.0 / math.sqrt(E)
        keys = rope(qkv[:, H * E:(H + 1) * E]).astype(jnp.bfloat16)
        values = qkv[:, (H + 1) * E:].astype(jnp.bfloat16)
        keep = mask_ref[...] > 0.5
        for h in range(H):
            q = rope(qkv[:, h * E:(h + 1) * E]).astype(jnp.bfloat16)
            s = lax.dot_general(q, keys, (((1,), (1,)), ((), ())), preferred_element_type=jnp.float32) * inv_sqrt
            s = jnp.where(keep, s, -jnp.inf)
            e = jnp.exp(s - jnp.max(s, axis=-1, keepdims=True))
            p = (e / jnp.sum(e, axis=-1, keepdims=True)).astype(jnp.bfloat16)
            ctx[:, h * E:(h + 1) * E] = jnp.dot(p, values, preferred_element_type=jnp.float32).astype(jnp.bfloat16)

    par_head = lax.rem(tp, 2)

    def kv_take(l, k):
        g = l * c.NC + k
        kv_copy(g).wait()
        slot = lax.rem(g, c.NR)

        def sub(s, _):
            r0 = pl.multiple_of(s * c.SUB, c.SUB)
            scr[...] = raw[slot, pl.ds(r0, c.SUB)].astype(jnp.float32).reshape(c.SUB * 4, LANES)
            for i in range(2):
                y = scr[pl.ds(2 * i + par_head, c.SUB, stride=4), :]
                wqkv[pl.ds(pl.multiple_of(k * c.KC + r0, c.SUB), c.SUB),
                     (H + i) * E:(H + 1 + i) * E] = y.astype(jnp.bfloat16)
            return 0

        lax.fori_loop(0, c.KC // c.SUB, sub, 0)

        @pl.when(g + c.NR < L * c.NC)
        def _():
            kv_copy(g + c.NR).start()

    def tables():
        def position(row):
            cls = jnp.where(row < HS, core, 1 - core)
            return (lax.shift_right_logical(row & (HS - 1), T.bit_length() - 1) * (2 * T)
                    + cls * T + (row & (T - 1)))

        pos = position(lax.broadcasted_iota(jnp.int32, (S, E), 0))
        lane = lax.broadcasted_iota(jnp.int32, (S, E), 1)
        pair_i = (lane & (E // 2 - 1)).astype(jnp.float32)
        ang = pos.astype(jnp.float32) * jnp.exp(pair_i * (-2.0 * math.log(ROPE_BASE) / E))
        cos_ref[...] = jnp.cos(ang)
        sin = jnp.sin(ang)
        sin_ref[...] = jnp.where(lane < E // 2, -sin, sin)
        kpos = position(lax.broadcasted_iota(jnp.int32, (S, S), 1))
        qpos = position(lax.broadcasted_iota(jnp.int32, (S, S), 0))
        mask_ref[...] = jnp.where(qpos >= kpos, 1.0, 0.0)

    for cp in inputs:
        cp.wait()
    resid[...] = hid_ref[...].astype(jnp.float32)
    norm_into(0, 0, na_ref)
    pl.semaphore_wait(bar, NZ)

    def layer(l, _):
        @pl.when(l > 0)
        def _():
            norm_into(l, 0, na_ref)

        def qkv_chunk(k):
            @pl.when(k == 0)
            def _():
                for h in range(H):
                    wq_copy(l, h).wait()
                qkv[...] = jnp.zeros_like(qkv)

            @pl.when(jnp.logical_and(l == 0, k == 0))
            def _():
                for n in range(c.NG):
                    for cp in gu_copies(n):
                        cp.start()
                for n in range(c.ND):
                    wd_copy(n).start()
            rows = pl.ds(pl.multiple_of(k * c.CKS[0], c.CKS[0]), c.CKS[0])
            qkv[...] += jnp.dot(xg[l, 0, :, kcols(0, k)], wqkv[rows, :], preferred_element_type=jnp.float32)

        def before():
            @pl.when(l == 0)
            def _():
                tables()
                lax.fori_loop(0, c.NC, lambda k, _: (kv_take(0, k), 0)[1], 0)
                wo_copy(0).start()

        gather_phase(l, 0, qkv_chunk, before)

        @pl.when(l + 1 < L)
        def _():
            for h in range(H):
                wq_copy(l + 1, h).start()
        attention()
        wo_copy(l).wait()

        def take_next(i):
            per = -(-c.NC // c.NN)
            for n in range(per):
                @pl.when(jnp.logical_and(l + 1 < L, i * per + n < c.NC))
                def _(n=n):
                    kv_take(l + 1, i * per + n)

        reduce_phase(l, 0, lambda j: jnp.dot(ctx[...], wo_b[:, ncols(j)], preferred_element_type=jnp.float32),
                     take_next)

        @pl.when(l + 1 < L)
        def _():
            wo_copy(l + 1).start()
        norm_into(l, 1, nm_ref)

        def gu_chunk(k):
            @pl.when(k == 0)
            def _():
                gacc[...] = jnp.zeros_like(gacc)
            g = l * c.NKS[1] + k
            slot = lax.rem(g, c.NG)
            for cp in gu_copies(g):
                cp.wait()
            gacc[...] += lax.dot_general(gu_b[slot], xg[l, 1, :, kcols(1, k)], (((1,), (1,)), ((), ())),
                                         preferred_element_type=jnp.float32)

            @pl.when(g + c.NG < L * c.NKS[1])
            def _():
                for cp in gu_copies(g + c.NG):
                    cp.start()

        gather_phase(l, 1, gu_chunk)
        gate = gacc[:c.F]
        act[...] = (gate * jax.nn.sigmoid(gate) * gacc[c.F:]).T.astype(jnp.bfloat16)

        def down_chunk(j):
            g = l * c.NN + j
            slot = lax.rem(g, c.ND)
            wd_copy(g).wait()
            part = jnp.dot(act[...], wd_b[slot], preferred_element_type=jnp.float32)

            @pl.when(g + c.ND < L * c.NN)
            def _():
                wd_copy(g + c.ND).start()
            return part

        reduce_phase(l, 1, down_chunk)
        return 0

    lax.fori_loop(0, L, layer, 0)
    out_ref[...] = resid[...].astype(jnp.bfloat16)


def solution(mesh):
    tok_spec = P('dp', 'tp', None)
    in_specs = (tok_spec, P(), P(None, None, 'tp', None), P(), P(None, 'tp', None, None), P(), P(None, None, 'tp'), P(None, None, 'tp'), P(None, 'tp', None))

    def body(hidden, norm_attn, w_q, w_kv, w_o, norm_mlp, w_gate, w_up, w_down):
        L, D, H, E = w_q.shape
        F = w_gate.shape[2]
        T = hidden.shape[1]
        S = 8 * T
        cfg = Cfg(L, S, D, H, E, F)
        c = cfg
        bf, f32 = jnp.bfloat16, jnp.float32
        vm = pl.BlockSpec(memory_space=pltpu.VMEM)
        hb = pl.BlockSpec(memory_space=pl.ANY)
        dma = pltpu.SemaphoreType.DMA
        mk = max(c.NKS)
        scratch = [
            pltpu.VMEM((L, 2, S, D), bf),
            pltpu.VMEM((L, 2, S // 2, D), bf),
            pltpu.VMEM((L, 2, NZ, T, D), bf),
            pltpu.VMEM((S // 2, D), bf),
            pltpu.VMEM((S // 2, D), bf),
            pltpu.VMEM((S // 2, D), f32),
            pltpu.VMEM((T, D), f32),
            pltpu.VMEM((D, (H + 2) * E), bf),
            pltpu.VMEM((c.NR, c.KC, 2, 2, E), bf),
            pltpu.VMEM((c.SUB * 4, E), f32),
            pltpu.VMEM((H * E, D), bf),
            pltpu.VMEM((c.NG, 2 * F, c.CKS[1]), bf),
            pltpu.VMEM((c.ND, F, c.CN), bf),
            pltpu.VMEM((S, (H + 2) * E), f32),
            pltpu.VMEM((2 * F, S), f32),
            pltpu.VMEM((S, F), bf),
            pltpu.VMEM((S, H * E), bf),
            pltpu.VMEM((T, D), bf), pltpu.VMEM((L, D), f32), pltpu.VMEM((L, D), f32),
            pltpu.VMEM((S, E), f32), pltpu.VMEM((S, E), f32), pltpu.VMEM((S, S), f32),
            dma((3,)),
            dma((H,)), dma((c.NR,)), dma, dma((c.NG, 2)), dma((c.ND,)),
            dma((L, 2, NZ, mk)), dma((L, 2, NZ, mk)), dma((5, mk)), dma((mk,)), dma((mk,)), dma((NZ, mk)),
            dma((L, 2, c.NN)), dma((L, 2, NZ, c.NN)), dma((c.NN,)), dma((NZ, c.NN)),
        ]
        out = pl.pallas_call(
            functools.partial(kernel, cfg),
            out_shape=jax.ShapeDtypeStruct((T, D), bf),
            in_specs=[hb] * 9,
            out_specs=vm,
            scratch_shapes=scratch,
            compiler_params=pltpu.CompilerParams(collective_id=0, has_side_effects=True, vmem_limit_bytes=67043328),
            name="layers",
        )(hidden[0], norm_attn, norm_mlp, jnp.transpose(w_q, (0, 2, 1, 3)), w_kv, w_o.reshape(L, H * E, D),
          jnp.transpose(w_gate, (0, 2, 1)), jnp.transpose(w_up, (0, 2, 1)), w_down)
        return out[None]

    return jax.shard_map(body, mesh=mesh, in_specs=in_specs, out_specs=tok_spec, check_vma=False)
```

```python
import functools
import math
import jax
import jax.numpy as jnp
from jax import lax
from jax.experimental import pallas as pl
from jax.experimental.pallas import tpu as pltpu
from jax.sharding import PartitionSpec as P

EPS = 1e-5
ROPE_BASE = 10000.0
MESH = pl.DeviceIdType.MESH
NZ = 4
LANES = 128


class Cfg:
    def __init__(self, layers, seq, width, heads, head, ff):
        self.L, self.S, self.D, self.H, self.E, self.F = layers, seq, width, heads, head, ff
        self.T = seq // 8
        self.CKS = (1280, 1024)
        self.NKS = tuple(width // n for n in self.CKS)
        self.KC = 512
        self.NC = width // self.KC
        self.CN = 1024
        self.NN = width // self.CN
        self.NG = 2
        self.ND = 4
        self.NR = 3
        self.SUB = 128
        self.AHEAD = (4, 3)
        self.LF, self.LP, self.LC = 0, 1, 2
        self.RP, self.RA, self.RB, self.RM, self.RS = 2, 3, 4, 4, 9


def kernel(cfg, hid_hbm, na_hbm, nm_hbm, wq_hbm, wkv_hbm, wo_hbm, wg_hbm, wu_hbm, wd_hbm, out_ref,
           xg, rsd, rsb, stg_d, stg_o, qb, resid, wqkv, raw, scr, wo_b, gu_b, wd_b,
           qkv, gacc, act, ctx, hid_ref, na_ref, nm_ref, cos_ref, sin_ref, mask_ref, s_in,
           s_wq, s_kv, s_wo, s_gu, s_wd,
           r_dir, r_par, s_own, s_far, s_near, s_par,
           q_par, q_dir, t_par, t_dir):
    c = cfg
    L, S, D, H, E, T = c.L, c.S, c.D, c.H, c.E, c.T
    HS = S // 2
    dp = lax.axis_index("dp")
    tp = lax.axis_index("tp")
    z = tp // 2
    core = lax.rem(tp, 2)
    partner = tp + 1 - 2 * core
    middle = jnp.logical_or(z == 1, z == 2)
    far = jnp.where(z == 1, 3, 0)
    near = jnp.where(z == 1, 0, 3)

    def chip(zz):
        return 2 * zz + core

    def rcopy(src, dst, ss, rs, to):
        return pltpu.make_async_remote_copy(src_ref=src, dst_ref=dst, send_sem=ss, recv_sem=rs,
                                            device_id=(dp, to), device_id_type=MESH)

    def blk(zz, base=0):
        return pl.ds(pl.multiple_of(base + zz * T, T), T)

    def kcols(ph, k):
        return pl.ds(pl.multiple_of(k * c.CKS[ph], c.CKS[ph]), c.CKS[ph])

    def ncols(j):
        return pl.ds(pl.multiple_of(j * c.CN, c.CN), c.CN)

    def wq_copy(l, h):
        return pltpu.make_async_copy(wq_hbm.at[l, h], wqkv.at[:, pl.ds(h * E, E)], s_wq.at[h])

    pair = pl.multiple_of(2 * (tp // 2), 2)

    def kv_copy(g):
        l, k, slot = g // c.NC, lax.rem(g, c.NC), lax.rem(g, c.NR)
        return pltpu.make_async_copy(
            wkv_hbm.at[l, pl.ds(pl.multiple_of(k * c.KC, c.KC), c.KC), :, pl.ds(pair, 2)],
            raw.at[slot], s_kv.at[slot])

    def wo_copy(l):
        return pltpu.make_async_copy(wo_hbm.at[l], wo_b, s_wo)

    def gu_copies(g):
        l, k, slot = g // c.NKS[1], lax.rem(g, c.NKS[1]), lax.rem(g, c.NG)
        return [pltpu.make_async_copy(w.at[l, :, kcols(1, k)], gu_b.at[slot, pl.ds(i * c.F, c.F)], s_gu.at[slot, i])
                for i, w in enumerate((wg_hbm, wu_hbm))]

    def wd_copy(g):
        l, j, slot = g // c.NN, lax.rem(g, c.NN), lax.rem(g, c.ND)
        return pltpu.make_async_copy(wd_hbm.at[l, :, ncols(j)], wd_b.at[slot], s_wd.at[slot])

    bar = pltpu.get_barrier_semaphore()
    pl.semaphore_signal(bar, inc=1, device_id=(dp, partner), device_id_type=MESH)
    for dz in (1, -1, 2, -2):
        @pl.when(jnp.logical_and(z + dz >= 0, z + dz < NZ))
        def _(dz=dz):
            pl.semaphore_signal(bar, inc=1, device_id=(dp, chip(z + dz)), device_id_type=MESH)

    inputs = [pltpu.make_async_copy(a, b, s_in.at[i])
              for i, (a, b) in enumerate(((hid_hbm, hid_ref), (na_hbm, na_ref), (nm_hbm, nm_ref)))]
    for cp in inputs:
        cp.start()
    for g in range(c.NR):
        kv_copy(g).start()
    for h in range(H):
        wq_copy(0, h).start()

    def gather_phase(l, ph, compute, before=None):
        buf = xg.at[l, ph]
        nk = c.NKS[ph]

        def own(k):
            src = buf.at[blk(z), kcols(ph, k)]
            res = [(None, rcopy(src, buf.at[blk(z, HS), kcols(ph, k)], s_own.at[0, k], r_par.at[l, ph, z, k], partner))]
            for i, dz in enumerate((2, -2, 1, -1)):
                ok = jnp.logical_and(z + dz >= 0, z + dz < NZ)
                if abs(dz) == 1:
                    late = jnp.logical_and(middle, z + dz == near)
                    ok = jnp.logical_and(ok, jnp.logical_not(late))
                to = chip(jnp.clip(z + dz, 0, NZ - 1))
                res.append((ok, rcopy(src, src, s_own.at[1 + i, k], r_dir.at[l, ph, z, k], to)))
            return res

        def near_send(k):
            b = buf.at[blk(z), kcols(ph, k)]
            return rcopy(b, b, s_near.at[k], r_dir.at[l, ph, z, k], chip(near))

        def dir_in(o, k):
            b = buf.at[blk(o), kcols(ph, k)]
            return rcopy(b, b, s_far.at[k], r_dir.at[l, ph, o, k], partner)

        def far_send(k):
            b = buf.at[blk(far), kcols(ph, k)]
            return rcopy(b, b, s_far.at[k], r_dir.at[l, ph, far, k], chip(near))

        def par_send(o, k):
            return rcopy(buf.at[blk(o), kcols(ph, k)], buf.at[blk(o, HS), kcols(ph, k)],
                         s_par.at[o, k], r_par.at[l, ph, o, k], partner)

        def start_own(k):
            for ok, cp in own(k):
                if ok is None:
                    cp.start()
                else:
                    @pl.when(ok)
                    def _(cp=cp):
                        cp.start()

        def stage_far(k):
            @pl.when(middle)
            def _():
                dir_in(far, k).wait_recv()
                far_send(k).start()
                near_send(k).start()

        def stage_par(k):
            for o in range(NZ):
                @pl.when(jnp.logical_and(o != z, jnp.logical_not(jnp.logical_and(middle, o == far))))
                def _(o=o):
                    dir_in(o, k).wait_recv()
                    par_send(o, k).start()

                @pl.when(jnp.logical_and(middle, o == far))
                def _(o=o):
                    par_send(o, k).start()

        def stage_in(k):
            for o in range(NZ):
                par_send(o, k).wait_recv()

        ahead = min(c.AHEAD[ph], nk)
        for k in range(ahead):
            start_own(k)

        if before is not None:
            before()

        def step(i, _):
            if ahead < nk:
                @pl.when(i + ahead < nk)
                def _():
                    start_own(i + ahead)

            @pl.when(jnp.logical_and(i >= c.LF, i < nk + c.LF))
            def _():
                stage_far(i - c.LF)

            @pl.when(jnp.logical_and(i >= c.LP, i < nk + c.LP))
            def _():
                stage_par(i - c.LP)

            @pl.when(i >= c.LC)
            def _():
                stage_in(i - c.LC)
                compute(i - c.LC)
            return 0

        lax.fori_loop(0, nk + c.LC, step, 0)

        def drain(k, _):
            for ok, cp in own(k):
                if ok is None:
                    cp.wait_send()
                else:
                    @pl.when(ok)
                    def _(cp=cp):
                        cp.wait_send()

            @pl.when(middle)
            def _():
                far_send(k).wait_send()
                near_send(k).wait_send()
            for o in range(NZ):
                @pl.when(o != z)
                def _(o=o):
                    par_send(o, k).wait_send()
            return 0

        lax.fori_loop(0, nk, drain, 0)

    def reduce_phase(l, ph, produce, beside=None):
        def par(j):
            return rcopy(stg_d.at[:, ncols(j)], rsd.at[l, ph, :, ncols(j)], t_par.at[j], q_par.at[l, ph, j], partner)

        def out(d, j):
            is_far = (z == 0) if d == 3 else (z == 3)
            if d in (0, 3):
                mid = 1 if d == 3 else 2
                to = jnp.where(is_far, mid, d)
                slot = jnp.where(is_far, mid, z)
                ok = jnp.logical_or(z == 0, z == 2) if d == 3 else jnp.logical_or(z == 1, z == 3)
            else:
                to, slot, ok = d, z, z != d
            return ok, rcopy(stg_o.at[blk(d), ncols(j)], rsb.at[l, ph, slot, :, ncols(j)],
                             t_dir.at[d, j], q_dir.at[l, ph, slot, j], chip(to))

        def mid_send(j):
            return rcopy(stg_o.at[blk(far), ncols(j)], rsb.at[l, ph, z, :, ncols(j)],
                         t_dir.at[far, j], q_dir.at[l, ph, z, j], chip(far))

        def dir_in(slot, j):
            b = rsb.at[l, ph, slot, :, ncols(j)]
            return rcopy(b, b, t_dir.at[0, j], q_dir.at[l, ph, slot, j], partner)

        def stage_make(j):
            part = produce(j)
            qb[:, ncols(j)] = part[:HS]
            stg_d[:, ncols(j)] = part[HS:].astype(jnp.bfloat16)
            par(j).start()

        def send(j, order, which):
            for d in order:
                ok, cp = out(d, j)

                @pl.when(jnp.logical_and(ok, which(d)))
                def _(cp=cp):
                    cp.start()

        def stage_pair(j):
            par(j).wait_recv()
            both = qb[:, ncols(j)] + rsd[l, ph, :, ncols(j)].astype(jnp.float32)
            qb[:, ncols(j)] = both
            stg_o[:, ncols(j)] = both.astype(jnp.bfloat16)
            send(j, (3, 0, 2, 1), lambda d: jnp.logical_or(middle, z == 3 - d) if d in (0, 3) else middle)

        def stage_mid(j):
            @pl.when(middle)
            def _():
                dir_in(z, j).wait_recv()
                both = qb[blk(far), ncols(j)] + rsb[l, ph, z, :, ncols(j)].astype(jnp.float32)
                stg_o[blk(far), ncols(j)] = both.astype(jnp.bfloat16)
                mid_send(j).start()

        def stage_sum(j):
            resid[:, ncols(j)] = resid[:, ncols(j)] + qb[blk(z), ncols(j)]
            for s in range(NZ):
                dist = jnp.abs(z - s)

                @pl.when(jnp.logical_and(dist >= 1, dist <= 2))
                def _(s=s):
                    dir_in(s, j).wait_recv()
                    resid[:, ncols(j)] = resid[:, ncols(j)] + rsb[l, ph, s, :, ncols(j)].astype(jnp.float32)

        def step(i, _):
            @pl.when(i < c.NN)
            def _():
                stage_make(i)

            @pl.when(jnp.logical_and(i >= c.RP, i < c.NN + c.RP))
            def _():
                stage_pair(i - c.RP)

            @pl.when(jnp.logical_and(i >= c.RA, i < c.NN + c.RA))
            def _():
                send(i - c.RA, (2, 1), lambda d: z == (0 if d == 2 else 3))

            @pl.when(jnp.logical_and(i >= c.RB, i < c.NN + c.RB))
            def _():
                send(i - c.RB, (1, 2), lambda d: z == (0 if d == 1 else 3))

            @pl.when(jnp.logical_and(i >= c.RM, i < c.NN + c.RM))
            def _():
                stage_mid(i - c.RM)

            if beside is not None:
                beside(i)

            @pl.when(i >= c.RS)
            def _():
                stage_sum(i - c.RS)
            return 0

        lax.fori_loop(0, c.NN + c.RS, step, 0)

        def drain(j, _):
            par(j).wait_send()
            for d in range(NZ):
                ok, cp = out(d, j)

                @pl.when(ok)
                def _(cp=cp):
                    cp.wait_send()

            @pl.when(middle)
            def _():
                mid_send(j).wait_send()
            return 0

        lax.fori_loop(0, c.NN, drain, 0)

    def norm_into(l, ph, gain_ref):
        r = resid[...]
        inv = lax.rsqrt(jnp.mean(r * r, axis=-1, keepdims=True) + EPS)
        xg[l, ph, blk(z), :] = (r * inv * gain_ref[pl.ds(l, 1), :]).astype(jnp.bfloat16)

    def rope(x):
        return x * cos_ref[...] + pltpu.roll(x, E // 2, 1) * sin_ref[...]

    def attention():
        inv_sqrt = 1.0 / math.sqrt(E)
        keys = rope(qkv[:, H * E:(H + 1) * E]).astype(jnp.bfloat16)
        values = qkv[:, (H + 1) * E:].astype(jnp.bfloat16)
        keep = mask_ref[...] > 0.5
        for h in range(H):
            q = rope(qkv[:, h * E:(h + 1) * E]).astype(jnp.bfloat16)
            s = lax.dot_general(q, keys, (((1,), (1,)), ((), ())), preferred_element_type=jnp.float32) * inv_sqrt
            s = jnp.where(keep, s, -jnp.inf)
            e = jnp.exp(s - jnp.max(s, axis=-1, keepdims=True))
            p = (e / jnp.sum(e, axis=-1, keepdims=True)).astype(jnp.bfloat16)
            ctx[:, h * E:(h + 1) * E] = jnp.dot(p, values, preferred_element_type=jnp.float32).astype(jnp.bfloat16)

    par_head = lax.rem(tp, 2)

    def kv_take(l, k):
        g = l * c.NC + k
        kv_copy(g).wait()
        slot = lax.rem(g, c.NR)

        def sub(s, _):
            r0 = pl.multiple_of(s * c.SUB, c.SUB)
            scr[...] = raw[slot, pl.ds(r0, c.SUB)].astype(jnp.float32).reshape(c.SUB * 4, LANES)
            for i in range(2):
                y = scr[pl.ds(2 * i + par_head, c.SUB, stride=4), :]
                wqkv[pl.ds(pl.multiple_of(k * c.KC + r0, c.SUB), c.SUB),
                     (H + i) * E:(H + 1 + i) * E] = y.astype(jnp.bfloat16)
            return 0

        lax.fori_loop(0, c.KC // c.SUB, sub, 0)

        @pl.when(g + c.NR < L * c.NC)
        def _():
            kv_copy(g + c.NR).start()

    def tables():
        def position(row):
            cls = jnp.where(row < HS, core, 1 - core)
            return (lax.shift_right_logical(row & (HS - 1), T.bit_length() - 1) * (2 * T)
                    + cls * T + (row & (T - 1)))

        pos = position(lax.broadcasted_iota(jnp.int32, (S, E), 0))
        lane = lax.broadcasted_iota(jnp.int32, (S, E), 1)
        pair_i = (lane & (E // 2 - 1)).astype(jnp.float32)
        ang = pos.astype(jnp.float32) * jnp.exp(pair_i * (-2.0 * math.log(ROPE_BASE) / E))
        cos_ref[...] = jnp.cos(ang)
        sin = jnp.sin(ang)
        sin_ref[...] = jnp.where(lane < E // 2, -sin, sin)
        kpos = position(lax.broadcasted_iota(jnp.int32, (S, S), 1))
        qpos = position(lax.broadcasted_iota(jnp.int32, (S, S), 0))
        mask_ref[...] = jnp.where(qpos >= kpos, 1.0, 0.0)

    for cp in inputs:
        cp.wait()
    resid[...] = hid_ref[...].astype(jnp.float32)
    norm_into(0, 0, na_ref)
    pl.semaphore_wait(bar, jnp.where(middle, NZ, NZ - 1))

    def layer(l, _):
        @pl.when(l > 0)
        def _():
            norm_into(l, 0, na_ref)

        def qkv_chunk(k):
            @pl.when(k == 0)
            def _():
                for h in range(H):
                    wq_copy(l, h).wait()
                qkv[...] = jnp.zeros_like(qkv)

            @pl.when(jnp.logical_and(l == 0, k == 0))
            def _():
                for n in range(c.NG):
                    for cp in gu_copies(n):
                        cp.start()
                for n in range(c.ND):
                    wd_copy(n).start()
            rows = pl.ds(pl.multiple_of(k * c.CKS[0], c.CKS[0]), c.CKS[0])
            qkv[...] += jnp.dot(xg[l, 0, :, kcols(0, k)], wqkv[rows, :], preferred_element_type=jnp.float32)

        def before():
            @pl.when(l == 0)
            def _():
                tables()
                lax.fori_loop(0, c.NC, lambda k, _: (kv_take(0, k), 0)[1], 0)
                wo_copy(0).start()

        gather_phase(l, 0, qkv_chunk, before)

        @pl.when(l + 1 < L)
        def _():
            for h in range(H):
                wq_copy(l + 1, h).start()
        attention()
        wo_copy(l).wait()

        def take_next(i):
            @pl.when(jnp.logical_and(l + 1 < L, i == c.RS - 1))
            def _():
                lax.fori_loop(0, c.NC, lambda k, _: (kv_take(l + 1, k), 0)[1], 0)

        reduce_phase(l, 0, lambda j: jnp.dot(ctx[...], wo_b[:, ncols(j)], preferred_element_type=jnp.float32),
                     take_next)

        @pl.when(l + 1 < L)
        def _():
            wo_copy(l + 1).start()
        norm_into(l, 1, nm_ref)

        def gu_chunk(k):
            @pl.when(k == 0)
            def _():
                gacc[...] = jnp.zeros_like(gacc)
            g = l * c.NKS[1] + k
            slot = lax.rem(g, c.NG)
            for cp in gu_copies(g):
                cp.wait()
            gacc[...] += lax.dot_general(gu_b[slot], xg[l, 1, :, kcols(1, k)], (((1,), (1,)), ((), ())),
                                         preferred_element_type=jnp.float32)

            @pl.when(g + c.NG < L * c.NKS[1])
            def _():
                for cp in gu_copies(g + c.NG):
                    cp.start()

        gather_phase(l, 1, gu_chunk)
        gate = gacc[:c.F]
        act[...] = (gate * jax.nn.sigmoid(gate) * gacc[c.F:]).astype(jnp.bfloat16).T

        def down_chunk(j):
            g = l * c.NN + j
            slot = lax.rem(g, c.ND)
            wd_copy(g).wait()
            part = jnp.dot(act[...], wd_b[slot], preferred_element_type=jnp.float32)

            @pl.when(g + c.ND < L * c.NN)
            def _():
                wd_copy(g + c.ND).start()
            return part

        reduce_phase(l, 1, down_chunk)
        return 0

    lax.fori_loop(0, L, layer, 0)
    out_ref[...] = resid[...].astype(jnp.bfloat16)


def solution(mesh):
    tok_spec = P('dp', 'tp', None)
    in_specs = (tok_spec, P(), P(None, None, 'tp', None), P(), P(None, 'tp', None, None), P(), P(None, None, 'tp'), P(None, None, 'tp'), P(None, 'tp', None))

    def body(hidden, norm_attn, w_q, w_kv, w_o, norm_mlp, w_gate, w_up, w_down):
        L, D, H, E = w_q.shape
        F = w_gate.shape[2]
        T = hidden.shape[1]
        S = 8 * T
        cfg = Cfg(L, S, D, H, E, F)
        c = cfg
        bf, f32 = jnp.bfloat16, jnp.float32
        vm = pl.BlockSpec(memory_space=pltpu.VMEM)
        hb = pl.BlockSpec(memory_space=pl.ANY)
        dma = pltpu.SemaphoreType.DMA
        mk = max(c.NKS)
        scratch = [
            pltpu.VMEM((L, 2, S, D), bf),
            pltpu.VMEM((L, 2, S // 2, D), bf),
            pltpu.VMEM((L, 2, NZ, T, D), bf),
            pltpu.VMEM((S // 2, D), bf),
            pltpu.VMEM((S // 2, D), bf),
            pltpu.VMEM((S // 2, D), f32),
            pltpu.VMEM((T, D), f32),
            pltpu.VMEM((D, (H + 2) * E), bf),
            pltpu.VMEM((c.NR, c.KC, 2, 2, E), bf),
            pltpu.VMEM((c.SUB * 4, E), f32),
            pltpu.VMEM((H * E, D), bf),
            pltpu.VMEM((c.NG, 2 * F, c.CKS[1]), bf),
            pltpu.VMEM((c.ND, F, c.CN), bf),
            pltpu.VMEM((S, (H + 2) * E), f32),
            pltpu.VMEM((2 * F, S), f32),
            pltpu.VMEM((S, F), bf),
            pltpu.VMEM((S, H * E), bf),
            pltpu.VMEM((T, D), bf), pltpu.VMEM((L, D), f32), pltpu.VMEM((L, D), f32),
            pltpu.VMEM((S, E), f32), pltpu.VMEM((S, E), f32), pltpu.VMEM((S, S), f32),
            dma((3,)),
            dma((H,)), dma((c.NR,)), dma, dma((c.NG, 2)), dma((c.ND,)),
            dma((L, 2, NZ, mk)), dma((L, 2, NZ, mk)), dma((5, mk)), dma((mk,)), dma((mk,)), dma((NZ, mk)),
            dma((L, 2, c.NN)), dma((L, 2, NZ, c.NN)), dma((c.NN,)), dma((NZ, c.NN)),
        ]
        out = pl.pallas_call(
            functools.partial(kernel, cfg),
            out_shape=jax.ShapeDtypeStruct((T, D), bf),
            in_specs=[hb] * 9,
            out_specs=vm,
            scratch_shapes=scratch,
            compiler_params=pltpu.CompilerParams(collective_id=0, has_side_effects=True, vmem_limit_bytes=67043328),
            name="layers",
        )(hidden[0], norm_attn, norm_mlp, jnp.transpose(w_q, (0, 2, 1, 3)), w_kv, w_o.reshape(L, H * E, D),
          jnp.transpose(w_gate, (0, 2, 1)), jnp.transpose(w_up, (0, 2, 1)), w_down)
        return out[None]

    return jax.shard_map(body, mesh=mesh, in_specs=in_specs, out_specs=tok_spec, check_vma=False)
```
